768 devices in a mesh: grp: 24 (over z, core), dev: 32 (over x, y).
Axes of the slice: x: 4, y: 8, z: 12, core: 2. Of those that a mesh axis runs over, the one named last changes fastest.
Arguments:
- positions: float32 [3, 3072, 544], P(None, ('grp', 'dev')), may hold values from -2 to 140, as said below
- rest_shape: float32 [3, 544], replicated, may hold values from -3 to 3
- stiffness: float32 [544, 544], replicated, may hold values from -0.25 to 0.25
- up_map: float32 [544, 152], replicated, may hold values from -0.25 to 0.25
- down_map: float32 [152, 544], replicated, may hold values from -0.5 to 0.5
- m2m: float32 [152, 152], replicated, may hold values from -0.5 to 0.5
- box_template: float32 [3, 152], replicated, may hold values from -1 to 1
- near_target: int32 [768, 2], P(('grp', 'dev')), may hold values from 0 to 3
- near_owner: int32 [768, 2], P(('grp', 'dev')), may hold values from 0 to 31, as said below
- near_cell: int32 [768, 2], P(('grp', 'dev')), may hold values from 0 to 3, as said below
- near_count: int32 [768], P(('grp', 'dev')), may hold values from 1 to 2, as said below
Outputs:
- new_positions: float32 [3, 3072, 544], P(None, ('grp', 'dev'))
- velocity: float32 [3, 3072, 544], P(None, ('grp', 'dev'))
The draws below stay inside these ranges and needn't reach their ends.
Inputs may be any that keep to these rules, and one draw needn't show every extreme that they name: `positions`: each cell's points lie within about 1.2 of the cell's center; devices of one group sit on a grid of spacing 2.5, groups are 6 apart. `near_owner`: device e's slots name devices of e's own group other than e itself; at most 2 used slots of one device name the same owner, and device 0 uses all 2 slots with exactly 2 on each owner it names. `near_cell`: the source cells named by one device's used slots are distinct. `near_count`: the used slots come first; device 0 uses all of them.
All inputs are finite; a program needn't handle non-finite values.
Results may differ from the reference program's by a relative error of at most 0.0003.
Values sent between devices are 32-bit elements; how exact they have to be, the bound alone decides.
A program may use at most 32 MiB of HBM per device.

```python
import jax
import jax.numpy as jnp
from jax import lax

P_SIZE = 544
Q = 152
CELLS_DEV = 4
NEAR = 2
CAP = 2
STEPS = 2
N_GRP = 24
N_DEV = 32


def near_lists(key):
    devices = N_GRP * N_DEV
    pair_count = NEAR // CAP
    key_owner, key_cell, key_order, key_count = jax.random.split(key, 4)
    device_ids = jnp.arange(devices, dtype=jnp.int32)
    scores = jax.random.randint(key_owner, (devices, N_DEV - 1), 0, 2 ** 20) * N_DEV + jnp.arange(N_DEV - 1, dtype=jnp.int32)[None, :]
    offsets = jnp.argsort(scores, axis=1)[:, :pair_count].astype(jnp.int32)
    owners = (device_ids[:, None] % N_DEV + 1 + offsets) % N_DEV
    owners = jnp.repeat(owners, CAP, axis=1)
    cell_scores = jax.random.randint(key_cell, (devices, pair_count, CELLS_DEV), 0, 2 ** 20) * CELLS_DEV + jnp.arange(CELLS_DEV, dtype=jnp.int32)[None, None, :]
    cell_ids = jnp.argsort(cell_scores, axis=2)[:, :, :CAP].reshape(devices, NEAR).astype(jnp.int32)
    order_scores = jax.random.randint(key_order, (devices, NEAR), 0, 2 ** 20) * NEAR + jnp.arange(NEAR, dtype=jnp.int32)[None, :]
    slot_order = jnp.argsort(order_scores, axis=1)
    owners = jnp.take_along_axis(owners, slot_order, axis=1).astype(jnp.int32)
    cell_ids = jnp.take_along_axis(cell_ids, slot_order, axis=1).astype(jnp.int32)
    counts = jax.random.randint(key_count, (devices,), 1, NEAR + 1).astype(jnp.int32)
    counts = counts.at[0].set(NEAR)
    return (owners, cell_ids, counts)


def draw_near_owner(key, part):
    return near_lists(jax.random.fold_in(key, 7))[0]


def draw_near_cell(key, part):
    return near_lists(jax.random.fold_in(key, 7))[1]


def draw_near_count(key, part):
    return near_lists(jax.random.fold_in(key, 7))[2]


def draw_positions(key, part):
    devices = N_GRP * N_DEV
    total = CELLS_DEV * devices
    cell_index = jnp.arange(total, dtype=jnp.int32)
    device_ids = cell_index // CELLS_DEV
    group_index = device_ids // N_DEV
    within = device_ids % N_DEV
    key_center, key_shape, key_rough = jax.random.split(jax.random.fold_in(key, 3), 3)
    grid = jnp.stack([2.5 * (within % 8).astype(jnp.float32), 2.5 * (within // 8).astype(jnp.float32), 6.0 * group_index.astype(jnp.float32)])
    centers = grid + jax.random.uniform(key_center, (3, total), jnp.float32, -0.5, 0.5)
    direction = jax.random.normal(key_shape, (3, total, P_SIZE), jnp.float32)
    direction = direction / jnp.sqrt(jnp.sum(direction * direction, axis=0, keepdims=True) + 0.1)
    roughness = 0.08 * jax.random.normal(key_rough, (3, total, P_SIZE), jnp.float32)
    return centers[:, :, None] + direction * (1.0 + roughness)


def with_ends(entries, rng, low, high):
    shape = entries.shape
    spot = [jax.random.randint(jax.random.fold_in(rng, axis), (), 0, shape[axis]) for axis in range(len(shape))]
    entries = entries.at[tuple(spot)].set(low)
    longest = shape.index(max(shape))
    spot[longest] = (spot[longest] + 1) % shape[longest]
    return entries.at[tuple(spot)].set(high)


def gaussian(own_key, dims, spread, most, held_as=jnp.bfloat16):
    values = spread * jax.random.normal(own_key, dims, jnp.float32)
    return jnp.clip(values, min=-most, max=most).astype(held_as)


def setup_inputs(seed: int = 0) -> dict:
    seeds = jax.random.split(jax.random.key(seed), 12)
    positions = draw_positions(jax.random.fold_in(seeds[11], 71), 0)
    rest_shape = gaussian(seeds[1], (3, P_SIZE), 0.5, 3.0, jnp.float32)
    stiffness = gaussian(seeds[2], (P_SIZE, P_SIZE), P_SIZE ** -0.5, 0.25, jnp.float32)
    up_map = gaussian(seeds[3], (P_SIZE, Q), P_SIZE ** -0.5, 0.25, jnp.float32)
    down_map = gaussian(seeds[4], (Q, P_SIZE), Q ** -0.5, 0.5, jnp.float32)
    m2m = gaussian(seeds[5], (Q, Q), Q ** -0.5, 0.5, jnp.float32)
    box_template = jnp.clip(jax.random.uniform(seeds[6], (3, Q), jnp.float32, -1.0, 1.0), -1.0, 1.0)
    near_target = with_ends(jax.random.randint(seeds[7], (N_GRP * N_DEV, NEAR), 0, CELLS_DEV), jax.random.fold_in(seeds[7], 1), 0, CELLS_DEV - 1).astype(jnp.int32)
    near_owner = draw_near_owner(jax.random.fold_in(seeds[11], 71), 0)
    near_cell = draw_near_cell(jax.random.fold_in(seeds[11], 71), 0)
    near_count = draw_near_count(jax.random.fold_in(seeds[11], 71), 0)
    return {"positions": positions, "rest_shape": rest_shape, "stiffness": stiffness, "up_map": up_map, "down_map": down_map, "m2m": m2m, "box_template": box_template, "near_target": near_target, "near_owner": near_owner, "near_cell": near_cell, "near_count": near_count}


EPSILON_SQ = 0.25
VISCOSITY = 0.039788735772973836
TIME_STEP = 0.1
SKALAK_HARDEN = 2.0
CHECK_RADIUS = 1.0
DEVICE_RADIUS = 1.5
GROUP_RADIUS = 6.0

def stokes(targets, sources, forces):
    delta_x = targets[0][:, None] - sources[0][None, :]
    delta_y = targets[1][:, None] - sources[1][None, :]
    delta_z = targets[2][:, None] - sources[2][None, :]
    square = delta_x * delta_x + delta_y * delta_y + delta_z * delta_z
    inverse = 1.0 / ((square + EPSILON_SQ) * jnp.sqrt(square + EPSILON_SQ))
    direct = (square + 2.0 * EPSILON_SQ) * inverse
    projected = (delta_x * forces[0][None, :] + delta_y * forces[1][None, :] + delta_z * forces[2][None, :]) * inverse
    result = jnp.einsum('ts,ks->kt', direct, forces, precision=lax.Precision.HIGHEST)
    extra = jnp.stack([lax.optimization_barrier(jnp.sum(delta_x * projected, axis=1)), lax.optimization_barrier(jnp.sum(delta_y * projected, axis=1)), lax.optimization_barrier(jnp.sum(delta_z * projected, axis=1))])
    return VISCOSITY * (result + extra)

def membrane(points, rest_shape, stiffness):
    centroid = lax.optimization_barrier(jnp.mean(points, axis=2, keepdims=True))
    strain = points - centroid - rest_shape[:, None, :]
    linear = jnp.dot(strain.reshape(-1, strain.shape[2]), stiffness, precision=lax.Precision.HIGHEST).reshape(strain.shape)
    stretch = lax.optimization_barrier(jnp.sum(linear * linear, axis=0))
    return -linear * (1.0 + SKALAK_HARDEN * stretch / (1.0 + stretch))

def box_far(checks, equivalents, centers, radius, weights, box_template):
    sources = centers[:, :, None] + radius * box_template[None]
    forces = equivalents * weights.astype(equivalents.dtype)[:, None, None]
    source_count = equivalents.shape[0] * equivalents.shape[2]
    flat_sources = jnp.transpose(sources, (1, 0, 2)).reshape(3, source_count)
    flat_forces = jnp.transpose(forces, (1, 0, 2)).reshape(3, source_count)
    return stokes(checks, flat_sources, flat_forces)

def reference(positions, rest_shape, stiffness, up_map, down_map, m2m, box_template, near_target, near_owner, near_cell, near_count):
    devices = N_GRP * N_DEV
    device_ids = jnp.arange(devices, dtype=jnp.int32)
    group_of = device_ids // N_DEV
    source_cells = ((group_of[:, None] * N_DEV + near_owner) * CELLS_DEV + near_cell).astype(jnp.int32)
    target_cells = (device_ids[:, None] * CELLS_DEV + near_target).astype(jnp.int32)
    in_use = jnp.arange(NEAR, dtype=jnp.int32)[None, :] < near_count[:, None]
    onehot = ((near_target[:, :, None] == jnp.arange(CELLS_DEV, dtype=jnp.int32)[None, None, :]) & in_use[:, :, None]).astype(positions.dtype)
    points = positions
    velocity = jnp.zeros_like(positions)
    for step_index in range(STEPS):
        forces = membrane(points, rest_shape, stiffness)
        by_points = points.reshape(3, devices, CELLS_DEV, P_SIZE)
        by_forces = forces.reshape(3, devices, CELLS_DEV, P_SIZE)
        summed = jnp.transpose(lax.optimization_barrier(jnp.sum(by_forces, axis=2)), (1, 0, 2)).reshape(devices * 3, P_SIZE)
        equivalents = jnp.dot(summed, up_map, precision=lax.Precision.HIGHEST).reshape(devices, 3, Q)
        centers = jnp.transpose(lax.optimization_barrier(jnp.mean(by_points, axis=(2, 3))))
        grouped = equivalents.reshape(N_GRP, N_DEV, 3, Q)
        placed = centers.reshape(N_GRP, N_DEV, 3)
        group_sums = lax.optimization_barrier(jnp.sum(grouped, axis=1)).reshape(N_GRP * 3, Q)
        group_eq = jnp.dot(group_sums, m2m, precision=lax.Precision.HIGHEST).reshape(N_GRP, 3, Q)
        group_centers = lax.optimization_barrier(jnp.mean(placed, axis=1))

        def far_one(device):
            group_index = device // N_DEV
            within = device % N_DEV
            checks = centers[device][:, None] + CHECK_RADIUS * box_template
            inner_far = box_far(checks, grouped[group_index], placed[group_index], DEVICE_RADIUS, jnp.arange(N_DEV, dtype=jnp.int32) != within, box_template)
            outer_far = box_far(checks, group_eq, group_centers, GROUP_RADIUS, jnp.arange(N_GRP, dtype=jnp.int32) != group_index, box_template)
            return inner_far + outer_far
        far_checks = lax.map(far_one, device_ids)
        far_surface = jnp.dot(far_checks.reshape(devices * 3, Q), down_map, precision=lax.Precision.HIGHEST).reshape(devices, 3, P_SIZE)
        stacked = jnp.concatenate([points, forces], axis=0)

        def near_one(device):
            sources = stacked[:, source_cells[device]]
            receivers = points[:, target_cells[device]]
            near_tiles = jax.vmap(stokes, in_axes=(1, 1, 1), out_axes=1)(receivers, sources[:3], sources[3:])
            return jnp.einsum('ksp,sc->kcp', near_tiles, onehot[device], precision=lax.Precision.HIGHEST)
        near_velocity = jnp.transpose(lax.map(near_one, device_ids), (1, 0, 2, 3))
        velocity = (jnp.transpose(far_surface, (1, 0, 2))[:, :, None, :] + near_velocity).reshape(3, CELLS_DEV * devices, P_SIZE)
        points = points + TIME_STEP * velocity
    return (points, velocity)
```

```python
import functools

import jax
import jax.numpy as jnp
from jax import lax
from jax.experimental import pallas as pl
from jax.experimental.pallas import tpu as pltpu
from jax.sharding import PartitionSpec as P

STEPS = 2
EPS = 0.25
VISCOSITY = 0.039788735772973836
TIME_STEP = 0.1
SKALAK_HARDEN = 2.0
CHECK_RADIUS = 1.0
DEVICE_RADIUS = 1.5
GROUP_RADIUS = 6.0

NG = 24
ND = 32
NX = 4
NY = 8
PT = 544
PP = 640
Q = 152
F32 = jnp.float32
BF = jnp.bfloat16
MESH = pl.DeviceIdType.MESH

EQ, GP, CA, CB, RQ = 0, 2, 4, 6, 8


def halves(w):
    hi = w.astype(BF)
    return hi, (w - hi.astype(F32)).astype(BF)


def dot(a, b):
    return jnp.dot(a, b, preferred_element_type=F32)


def mm(a, hi, lo):
    ah, al = halves(a)
    return dot(ah, hi[...]) + dot(al, hi[...]) + dot(ah, lo[...])


def pair(t, s, acc):
    tx, ty, tz = t
    sx, sy, sz, fx, fy, fz = s
    dx, dy, dz = tx - sx, ty - sy, tz - sz
    rs = lax.rsqrt(dx * dx + dy * dy + (dz * dz + EPS))
    b = rs * rs * rs
    direct = rs + EPS * b
    proj = (dx * fx + dy * fy + dz * fz) * b
    return (
        acc[0] + (direct * fx + proj * dx),
        acc[1] + (direct * fy + proj * dy),
        acc[2] + (direct * fz + proj * dz),
    )


def row_of(tile, j, rows):
    return jnp.broadcast_to(tile[j : j + 1, :], (rows, 128))


def kernel(
    near_target,
    near_owner,
    near_cell,
    near_count,
    pos_ref,
    rest_ref,
    stiff_ref,
    up_ref,
    m2m_ref,
    down_ref,
    cols_ref,
    rows_ref,
    new_ref,
    vel_ref,
    st_hi,
    st_lo,
    up_hi,
    up_lo,
    mm_hi,
    mm_lo,
    dn_hi,
    dn_lo,
    targets,
    acc_ref,
    eq_buf,
    gp_buf,
    ca_buf,
    cb_send,
    cb_recv,
    rq_send,
    rq_recv,
    src_dev,
    src_grp,
    near_src,
    near_rows,
    near_cols,
    near_acc,
    send_sem,
    recv_sem,
):
    me = lax.axis_index("dev")
    grp = lax.axis_index("grp")
    mx = me // NY
    my = me % NY

    barrier = pltpu.get_barrier_semaphore()

    def greet(axis, own, count):
        def one(i, c):
            pl.semaphore_signal(
                barrier, inc=1, device_id={axis: lax.rem(own + i, count)}, device_id_type=MESH
            )
            return c

        lax.fori_loop(1, count, one, 0)

    greet("dev", me, ND)
    greet("grp", grp, NG)

    def push(src, dst, sem, device):
        pltpu.make_async_remote_copy(
            src_ref=src,
            dst_ref=dst,
            send_sem=send_sem.at[sem],
            recv_sem=recv_sem.at[sem],
            device_id=device,
            device_id_type=MESH,
        ).start()

    def arrived(ref, sem):
        pltpu.make_async_copy(ref, ref, recv_sem.at[sem]).wait()

    def left(ref, sem):
        pltpu.make_async_copy(ref, ref, send_sem.at[sem]).wait()

    def push_all(buf, base, rows, axis, own, count, sem):
        slot = buf.at[pl.ds(pl.multiple_of(base + own * rows, 8), rows), :]

        def one(i, c):
            push(slot, slot, sem, {axis: lax.rem(own + i, count)})
            return c

        lax.fori_loop(1, count, one, 0)

    st_hi[...], st_lo[...] = halves(stiff_ref[...])
    up_hi[...], up_lo[...] = halves(up_ref[...])
    mm_hi[...], mm_lo[...] = halves(m2m_ref[...])
    dn_hi[...], dn_lo[...] = halves(down_ref[...])
    for k in range(3):
        targets[k * Q : (k + 1) * Q, :] = jnp.broadcast_to(
            CHECK_RADIUS * cols_ref[:, k : k + 1], (Q, 128)
        )
    near_src[...] = jnp.zeros_like(near_src)
    near_rows[...] = jnp.zeros_like(near_rows)
    near_acc[...] = jnp.zeros_like(near_acc)

    sub = lax.broadcasted_iota(jnp.int32, (8, 128), 0)
    lane = lax.broadcasted_iota(jnp.int32, (8, 128), 1)
    row8 = lax.broadcasted_iota(jnp.int32, (8, PT), 0)
    count = near_count[0]
    t_of = [near_target[0, s] for s in range(2)]
    used = [s < count for s in range(2)]

    want, from_y = [], []
    for s in range(2):
        owner = near_owner[0, s]
        want.append((owner // NY) * 16 + near_cell[0, s])
        from_y.append(jnp.where(used[s], owner % NY, -1))
    kk = sub % 4
    slot_want = jnp.where(sub < 4, want[0], want[1]) + 4 * kk
    slot_y = jnp.where(sub < 4, from_y[0], from_y[1])
    for y in range(NY):
        rq_send[y * 8 : (y + 1) * 8, :] = jnp.where((slot_y == y) & (kk < 3), slot_want, -1)

    def membrane(pts):
        cents, strain = [], []
        for k in range(3):
            c = jnp.sum(pts[k], axis=1, keepdims=True) * (1.0 / PT)
            cents.append(c)
            strain.append(pts[k] - c - rest_ref[k : k + 1, :])
        flat = jnp.concatenate(strain, axis=0)
        hi = flat.astype(BF).astype(F32)
        both = jnp.concatenate([hi, flat - hi], axis=0).astype(BF)
        first = dot(both, st_hi[...])
        linear = first[:24] + first[24:] + dot(both[:32], st_lo[...])[:24]
        lin = [linear[8 * k : 8 * k + 8] for k in range(3)]
        stretch = lin[0] * lin[0] + lin[1] * lin[1] + lin[2] * lin[2]
        harden = 1.0 + SKALAK_HARDEN * stretch / (1.0 + stretch)
        return cents, [-l * harden for l in lin]

    def own_cells(pts):
        return jnp.concatenate([p[:4] for p in pts] + [jnp.zeros((4, PT), F32)], axis=0)

    def sources(src, buf, base, boxes, rem_rows, own, radius, center):
        total = boxes + 8
        mine = lax.broadcasted_iota(jnp.int32, (boxes, 128), 0) == own
        middle = buf[pl.ds(base + 6, boxes, stride=8), :]
        for k in range(3):
            f = buf[pl.ds(base + k, boxes, stride=8), :]
            src[(3 + k) * total : (3 + k) * total + boxes, :] = jnp.where(mine, 0.0, f * VISCOSITY)
            r = buf[pl.ds(base + 3 + k, boxes, stride=8), :]
            r = jnp.where(mine, 0.0, r * VISCOSITY)
            packed = r[0:8]
            for j in range(1, boxes // 8):
                packed = packed + r[8 * j : 8 * j + 8]
            src[(3 + k) * total + boxes : (4 + k) * total, :] = packed
            c = jnp.broadcast_to(middle[:, k : k + 1] - center[k], (boxes, 128))
            src[k * total : k * total + boxes, :] = c + radius * rows_ref[k : k + 1, :128]
            pc = c[0:8]
            for j in range(1, boxes // 8):
                pc = jnp.where(lane // 32 == j, c[8 * j : 8 * j + 8], pc)
            src[k * total + boxes : (k + 1) * total, :] = pc + radius * rows_ref[k : k + 1, 128:]

    def far(src, boxes, first):
        total = boxes + 8
        edges = [0, 24, 48, 72, 96, 120, 152]
        for lo, hi in zip(edges[:-1], edges[1:]):
            n = hi - lo
            t = [targets[k * Q + lo : k * Q + hi, :] for k in range(3)]
            if first:
                acc = tuple(jnp.zeros((n, 128), F32) for k in range(3))
            else:
                acc = tuple(acc_ref[k * Q + lo : k * Q + hi, :] for k in range(3))

            def one(c, acc):
                tiles = [
                    src[pl.ds(pl.multiple_of(k * total + c * 8, 8), 8), :] for k in range(6)
                ]
                for j in range(8):
                    acc = pair(t, [row_of(x, j, n) for x in tiles], acc)
                return acc

            acc = lax.fori_loop(0, total // 8, one, acc)
            for k in range(3):
                acc_ref[k * Q + lo : k * Q + hi, :] = acc[k]

    pts = [pos_ref[8 * k : 8 * k + 8, :] for k in range(3)]
    for step in range(STEPS):
        eq0, gp0, ca0, cb0 = step * 256, step * 192, step * 64, step * 64
        cents, forces = membrane(pts)
        center = [jnp.sum(c[:4], axis=0, keepdims=True) * 0.25 for c in cents]
        total = [jnp.sum(f[:4], axis=0, keepdims=True) for f in forces]
        m3 = row8 % 3
        fs = jnp.where(m3 == 0, total[0], jnp.where(m3 == 1, total[1], total[2]))
        e = mm(fs, up_hi, up_lo)
        mid = jnp.where(lane == 0, center[0], jnp.where(lane == 1, center[1], center[2]))
        msg = jnp.where(
            sub < 3,
            e[:, :128],
            jnp.where(
                sub < 6,
                jnp.where(lane // 32 == mx, e[:, 128:], 0.0),
                jnp.where(sub == 6, mid, 0.0),
            ),
        )
        eq_buf[pl.ds(pl.multiple_of(eq0 + me * 8, 8), 8), :] = msg
        ca_buf[pl.ds(pl.multiple_of(ca0 + mx * 16, 8), 16), :] = own_cells(pts)

        if step == 0:
            pl.semaphore_wait(barrier, ND - 1 + NG - 1)
        push_all(eq_buf, eq0, 8, "dev", me, ND, EQ + step)

        cells = ca_buf.at[pl.ds(pl.multiple_of(ca0 + mx * 16, 8), 16), :]
        for i in range(1, NX):
            push(cells, cells, CA + step, {"dev": lax.rem(mx + i, NX) * NY + my})
        mine = pl.ds(pl.multiple_of(my * 8, 8), 8)
        if step == 0:
            for i in range(1, NY):
                y = lax.rem(my + i, NY)
                push(
                    rq_send.at[pl.ds(pl.multiple_of(y * 8, 8), 8), :],
                    rq_recv.at[mine, :],
                    RQ,
                    {"dev": mx * NY + y},
                )
            rq_recv[mine, :] = rq_send[mine, :]
            arrived(rq_recv.at[pl.ds(0, 56), :], RQ)

        arrived(ca_buf.at[pl.ds(ca0, 48), :], CA + step)
        pick = rq_recv[:, :64] == lax.broadcasted_iota(jnp.int32, (64, 64), 1)
        pick = jnp.where(pick, 1.0, 0.0).astype(BF)
        cells = ca_buf[ca0 : ca0 + 64, :]
        c1 = cells.astype(BF)
        cells = cells - c1.astype(F32)
        c2 = cells.astype(BF)
        c3 = (cells - c2.astype(F32)).astype(BF)
        cb_send[cb0 : cb0 + 64, :] = (dot(pick, c1) + dot(pick, c2)) + dot(pick, c3)
        own_b = pl.ds(pl.multiple_of(cb0 + my * 8, 8), 8)
        for i in range(1, NY):
            y = lax.rem(my + i, NY)
            push(
                cb_send.at[pl.ds(pl.multiple_of(cb0 + y * 8, 8), 8), :],
                cb_recv.at[own_b, :],
                CB + step,
                {"dev": mx * NY + y},
            )
        cb_recv[own_b, :] = cb_send[own_b, :]

        arrived(eq_buf.at[pl.ds(eq0, 248), :], EQ + step)
        parts = [eq_buf[eq0 + 8 * i : eq0 + 8 * i + 8, :] for i in range(ND)]
        while len(parts) > 1:
            parts = [a + b for a, b in zip(parts[::2], parts[1::2])]
        tile = parts[0]
        th, tl = halves(tile)
        up1 = dot(th, mm_hi[:128]) + dot(tl, mm_hi[:128]) + dot(th, mm_lo[:128])
        up2 = dot(th, mm_hi[128:]) + dot(tl, mm_hi[128:]) + dot(th, mm_lo[128:])
        main = up1[:, :128] + pltpu.roll(up2[:, :128], 5, 0)
        rest = pltpu.roll(up1[:, 128:], 3, 0) + up2[:, 128:]
        msg = jnp.where(
            sub < 3,
            main,
            jnp.where(
                sub < 6, jnp.where(lane // 32 == grp // 8, rest, 0.0), tile * (1.0 / ND)
            ),
        )
        gp_buf[pl.ds(pl.multiple_of(gp0 + grp * 8, 8), 8), :] = msg
        push_all(gp_buf, gp0, 8, "grp", grp, NG, GP + step)

        sources(src_dev, eq_buf, eq0, ND, 8, me, DEVICE_RADIUS, center)
        far(src_dev, ND, True)

        arrived(cb_recv.at[pl.ds(cb0, 56), :], CB + step)
        near = cb_recv[cb0 : cb0 + 8, :]
        for y in range(1, NY):
            near = near + cb_recv[cb0 + 8 * y : cb0 + 8 * y + 8, :]
        npts = [jnp.where(row8 == 0, near[k : k + 1], near[4 + k : 5 + k]) for k in range(3)]
        _, nforces = membrane(npts)
        for s in range(2):
            for k in range(3):
                near_src[s * 8 + k : s * 8 + k + 1, :PT] = near[4 * s + k : 4 * s + k + 1]
                near_src[s * 8 + 3 + k : s * 8 + 4 + k, :PT] = nforces[k][s : s + 1] * VISCOSITY
                near_rows[4 * s + k : 4 * s + k + 1, :PT] = jnp.sum(
                    jnp.where(row8 == t_of[s], pts[k], 0.0), axis=0, keepdims=True
                )
        near_cols[...] = near_rows[...].T

        def near_block(i, c):
            at = pl.multiple_of(i * 32, 32)
            cols = near_cols[pl.ds(at, 32), :]
            for s in range(2):
                t = [
                    jnp.broadcast_to(cols[:, 4 * s + k : 4 * s + k + 1], (32, 128))
                    for k in range(3)
                ]
                acc = tuple(jnp.zeros((32, 128), F32) for k in range(3))
                for q in range(PP // 128):
                    src = near_src[s * 8 : s * 8 + 8, q * 128 : q * 128 + 128]
                    acc = pair(t, [row_of(src, j, 32) for j in range(6)], acc)
                for k in range(3):
                    near_acc[pl.ds((3 * s + k) * PP + at, 32), :] = acc[k]
            return c

        lax.fori_loop(0, PT // 32, near_block, 0)
        nv = []
        for i in range(6):
            summed = jnp.sum(near_acc[i * PP : (i + 1) * PP, :].T, axis=0, keepdims=True)
            nv.append(summed[:, :PT])

        arrived(gp_buf.at[pl.ds(gp0, 184), :], GP + step)
        sources(src_grp, gp_buf, gp0, NG, 8, grp, GROUP_RADIUS, center)
        far(src_grp, NG, False)
        ones = jnp.ones((16, 128), BF)
        checks = []
        for k in range(3):
            ah, al = halves(acc_ref[k * Q : (k + 1) * Q, :])
            dims = (((1,), (1,)), ((), ()))
            checks.append(
                (
                    lax.dot_general(ones, ah, dims, preferred_element_type=F32)
                    + lax.dot_general(ones, al, dims, preferred_element_type=F32)
                )[:8]
            )
        surface = mm(jnp.concatenate(checks, axis=0), dn_hi, dn_lo)

        for k in range(3):
            v = surface[8 * k : 8 * k + 8]
            for s in range(2):
                v = v + jnp.where((row8 == t_of[s]) & used[s], nv[3 * s + k], 0.0)
            pts[k] = pts[k] + TIME_STEP * v
            if step == STEPS - 1:
                vel_ref[8 * k : 8 * k + 8, :] = v
                new_ref[8 * k : 8 * k + 8, :] = pts[k]

    for step in range(STEPS):
        left(eq_buf.at[pl.ds(0, 248), :], EQ + step)
        left(gp_buf.at[pl.ds(0, 184), :], GP + step)
        left(ca_buf.at[pl.ds(0, 48), :], CA + step)
        left(cb_send.at[pl.ds(0, 56), :], CB + step)
    left(rq_send.at[pl.ds(0, 56), :], RQ)


def body(
    positions,
    rest_shape,
    stiffness,
    up_map,
    down_map,
    m2m,
    box_template,
    near_target,
    near_owner,
    near_cell,
    near_count,
):
    def spread(a):
        gap = jnp.zeros((a.shape[0], 8), F32)
        rest = a[:, 128:]
        return jnp.concatenate([a[:, :128]] + [rest, gap] * 4, axis=1)

    padded = jnp.pad(positions, ((0, 0), (0, 4), (0, 0))).reshape(24, PT)
    m2 = spread(spread(m2m).T).T
    vmem = pl.BlockSpec(memory_space=pltpu.VMEM)
    smem = pl.BlockSpec(memory_space=pltpu.SMEM)
    shape = jax.ShapeDtypeStruct((24, PT), F32)
    new, vel = pl.pallas_call(
        kernel,
        out_shape=(shape, shape),
        in_specs=[smem] * 4 + [vmem] * 8,
        out_specs=(vmem, vmem),
        scratch_shapes=[
            pltpu.VMEM((PT, PT), BF),
            pltpu.VMEM((PT, PT), BF),
            pltpu.VMEM((PT, 256), BF),
            pltpu.VMEM((PT, 256), BF),
            pltpu.VMEM((256, 256), BF),
            pltpu.VMEM((256, 256), BF),
            pltpu.VMEM((Q, PT), BF),
            pltpu.VMEM((Q, PT), BF),
            pltpu.VMEM((3 * Q, 128), F32),
            pltpu.VMEM((3 * Q, 128), F32),
            pltpu.VMEM((STEPS * 256, 128), F32),
            pltpu.VMEM((STEPS * 192, 128), F32),
            pltpu.VMEM((STEPS * 64, PT), F32),
            pltpu.VMEM((STEPS * 64, PT), F32),
            pltpu.VMEM((STEPS * 64, PT), F32),
            pltpu.VMEM((64, 128), jnp.int32),
            pltpu.VMEM((64, 128), jnp.int32),
            pltpu.VMEM((6 * 40, 128), F32),
            pltpu.VMEM((6 * 32, 128), F32),
            pltpu.VMEM((16, PP), F32),
            pltpu.VMEM((8, PP), F32),
            pltpu.VMEM((PP, 8), F32),
            pltpu.VMEM((6 * PP, 128), F32),
            pltpu.SemaphoreType.DMA((9,)),
            pltpu.SemaphoreType.DMA((9,)),
        ],
        compiler_params=pltpu.CompilerParams(
            collective_id=0, has_side_effects=True, vmem_limit_bytes=40 * 1024 * 1024
        ),
    )(
        near_target,
        near_owner,
        near_cell,
        near_count,
        padded,
        rest_shape,
        stiffness,
        spread(up_map),
        m2,
        down_map,
        box_template.T,
        spread(box_template),
    )
    return (
        new.reshape(3, 8, PT)[:, :4],
        vel.reshape(3, 8, PT)[:, :4],
    )


def solution(mesh):
    return jax.shard_map(
        body,
        mesh=mesh,
        in_specs=(
            P(None, ("grp", "dev"), None),
            P(),
            P(),
            P(),
            P(),
            P(),
            P(),
            P(("grp", "dev"), None),
            P(("grp", "dev"), None),
            P(("grp", "dev"), None),
            P(("grp", "dev")),
        ),
        out_specs=(P(None, ("grp", "dev"), None), P(None, ("grp", "dev"), None)),
        check_vma=False,
    )
```

```python
import functools

import jax
import jax.numpy as jnp
from jax import lax
from jax.experimental import pallas as pl
from jax.experimental.pallas import tpu as pltpu
from jax.sharding import PartitionSpec as P

STEPS = 2
EPS = 0.25
VISCOSITY = 0.039788735772973836
TIME_STEP = 0.1
SKALAK_HARDEN = 2.0
CHECK_RADIUS = 1.0
DEVICE_RADIUS = 1.5
GROUP_RADIUS = 6.0

NG = 24
ND = 32
NX = 4
NY = 8
PT = 544
PP = 640
Q = 152
F32 = jnp.float32
BF = jnp.bfloat16
MESH = pl.DeviceIdType.MESH

QP = 160
DEV_OFF = sorted(
    [(x, y) for x in range(NX) for y in range(NY) if (x, y) != (0, 0)],
    key=lambda o: (min(o[0], NX - o[0]) + min(o[1], NY - o[1]), o),
)
GRP_OFF = sorted(range(1, NG), key=lambda o: (min(o, NG - o), o))
DEV_SLOT = {o: i for i, o in enumerate(DEV_OFF)}
GRP_SLOT = {o: i for i, o in enumerate(GRP_OFF)}
EQ, GP, CA, CB, RQ = 0, 8, 14, 16, 18


def halves(w):
    hi = w.astype(BF)
    return hi, (w - hi.astype(F32)).astype(BF)


def dot(a, b):
    return jnp.dot(a, b, preferred_element_type=F32)


def dot_t(a, b):
    return lax.dot_general(a, b, (((1,), (1,)), ((), ())), preferred_element_type=F32)


def mm(a, hi, lo):
    ah, al = halves(a)
    return dot(ah, hi[...]) + dot(al, hi[...]) + dot(ah, lo[...])


def pair(t, s, acc):
    tx, ty, tz = t
    sx, sy, sz, fx, fy, fz = s
    dx, dy, dz = tx - sx, ty - sy, tz - sz
    rs = lax.rsqrt(dx * dx + dy * dy + (dz * dz + EPS))
    b = rs * rs * rs
    direct = rs + EPS * b
    proj = (dx * fx + dy * fy + dz * fz) * b
    return (
        acc[0] + (direct * fx + proj * dx),
        acc[1] + (direct * fy + proj * dy),
        acc[2] + (direct * fz + proj * dz),
    )


def row_of(tile, j, rows):
    return jnp.broadcast_to(tile[j : j + 1, :], (rows, 128))


def kernel(
    *refs
):
    inputs, (new_ref, vel_ref), local = refs[:11], refs[11:13], refs[13:24]
    (
        st_hi,
        st_lo,
        up_hi,
        up_lo,
        mm_hi,
        mm_lo,
        dn_hi,
        dn_lo,
        box_rows,
        targets,
        acc_ref,
        eq_msg,
        gp_msg,
        eq_buf,
        gp_buf,
        ca_buf,
        cb_send,
        cb_recv,
        rq_send,
        rq_recv,
        src_ref,
        near_src,
        near_rows,
        near_cols,
        near_acc,
        send_sem,
        recv_sem,
        load_sem,
    ) = refs[24:]
    loads = [
        pltpu.make_async_copy(a, b, load_sem.at[i])
        for i, (a, b) in enumerate(zip(inputs, local))
    ]
    for load in loads:
        load.start()
    (
        near_target,
        near_owner,
        near_cell,
        near_count,
        pos_ref,
        rest_ref,
        stiff_ref,
        up_ref,
        m2m_ref,
        down_ref,
        box_ref,
    ) = local
    me = lax.axis_index("dev")
    grp = lax.axis_index("grp")
    mx = me // NY
    my = me % NY

    barrier = pltpu.get_barrier_semaphore()

    def greet(axis, own, count):
        def one(i, c):
            pl.semaphore_signal(
                barrier, inc=1, device_id={axis: lax.rem(own + i, count)}, device_id_type=MESH
            )
            return c

        lax.fori_loop(1, count, one, 0)

    greet("dev", me, ND)
    greet("grp", grp, NG)

    def push(src, dst, sem, device, arrival=None):
        pltpu.make_async_remote_copy(
            src_ref=src,
            dst_ref=dst,
            send_sem=send_sem.at[sem],
            recv_sem=recv_sem.at[sem if arrival is None else arrival],
            device_id=device,
            device_id_type=MESH,
        ).start()

    def arrived(ref, sem):
        pltpu.make_async_copy(ref, ref, recv_sem.at[sem]).wait()

    def left(ref, sem):
        pltpu.make_async_copy(ref, ref, send_sem.at[sem]).wait()

    def send_boxes(step):
        for x, y in reversed(DEV_OFF):
            slot = DEV_SLOT[((NX - x) % NX, (NY - y) % NY)]
            peer = lax.rem(mx + x, NX) * NY + lax.rem(my + y, NY)
            push(
                eq_msg.at[step],
                eq_buf.at[step * 32 + slot],
                EQ + 4 * step,
                {"dev": peer},
                EQ + 4 * step + slot // 8,
            )

    def send_groups(step):
        for o in reversed(GRP_OFF):
            slot = GRP_SLOT[NG - o]
            push(
                gp_msg.at[step],
                gp_buf.at[step * 24 + slot],
                GP + 3 * step,
                {"grp": lax.rem(grp + o, NG)},
                GP + 3 * step + slot // 8,
            )

    for load in loads:
        load.wait()

    def spread(a, axis):
        shape = list(a.shape)
        shape[axis] = 8
        gap = jnp.zeros(shape, F32)
        main, rest = (a[:, :128], a[:, 128:]) if axis else (a[:128], a[128:])
        return jnp.concatenate([main] + [rest, gap] * 4, axis=axis)

    st_hi[...], st_lo[...] = halves(stiff_ref[...])
    up_hi[...], up_lo[...] = halves(spread(up_ref[...], 0))
    mm_hi[0:Q, :], mm_lo[0:Q, :] = halves(spread(m2m_ref[...], 1))
    mm_hi[Q:, :] = jnp.zeros((8, 256), BF)
    mm_lo[Q:, :] = jnp.zeros((8, 256), BF)
    dn_hi[...], dn_lo[...] = halves(down_ref[...])
    box_rows[...] = jnp.zeros_like(box_rows)
    box_rows[0:3, 0:Q] = box_ref[...]
    cols = box_rows[...].T
    for k in range(3):
        targets[k * QP : (k + 1) * QP, :] = jnp.broadcast_to(
            CHECK_RADIUS * cols[:QP, k : k + 1], (QP, 128)
        )
    box_rows[0:3, :] = spread(box_ref[...], 1)
    for step in range(STEPS):
        eq_buf[step * 32 + 31] = jnp.zeros((4, 128), F32)
        gp_buf[step * 24 + 23] = jnp.zeros((4, 128), F32)
    near_src[...] = jnp.zeros_like(near_src)
    near_rows[...] = jnp.zeros_like(near_rows)
    near_acc[...] = jnp.zeros_like(near_acc)

    sub = lax.broadcasted_iota(jnp.int32, (8, 128), 0)
    lane = lax.broadcasted_iota(jnp.int32, (8, 128), 1)
    row8 = lax.broadcasted_iota(jnp.int32, (8, PT), 0)
    count = near_count[0]
    t_of = [near_target[0, s] for s in range(2)]
    used = [s < count for s in range(2)]

    want, from_y = [], []
    for s in range(2):
        owner = near_owner[0, s]
        want.append((owner // NY) * 16 + near_cell[0, s])
        from_y.append(jnp.where(used[s], owner % NY, -1))
    kk = sub % 4
    slot_want = jnp.where(sub < 4, want[0], want[1]) + 4 * kk
    slot_y = jnp.where(sub < 4, from_y[0], from_y[1])
    for y in range(NY):
        rq_send[y * 8 : (y + 1) * 8, :] = jnp.where((slot_y == y) & (kk < 3), slot_want, -1)

    def membrane(pts):
        cents, strain = [], []
        for k in range(3):
            c = jnp.sum(pts[k], axis=1, keepdims=True) * (1.0 / PT)
            cents.append(c)
            strain.append(pts[k] - c - rest_ref[k : k + 1, :])
        flat = jnp.concatenate(strain, axis=0)
        hi = flat.astype(BF).astype(F32)
        both = jnp.concatenate([hi, flat - hi], axis=0).astype(BF)
        first = dot(both, st_hi[...])
        linear = first[:24] + first[24:] + dot(both[:32], st_lo[...])[:24]
        lin = [linear[8 * k : 8 * k + 8] for k in range(3)]
        stretch = lin[0] * lin[0] + lin[1] * lin[1] + lin[2] * lin[2]
        harden = 1.0 + SKALAK_HARDEN * stretch / (1.0 + stretch)
        return cents, [-l * harden for l in lin]

    def own_cells(pts):
        return jnp.concatenate([p[:4] for p in pts] + [jnp.zeros((4, PT), F32)], axis=0)

    def message(e, center):
        rest = jnp.where(lane == 96, center[0], jnp.where(lane == 97, center[1], center[2]))
        for k in range(3):
            rest = jnp.where(lane // 32 == k, e[k : k + 1, 128:], rest)
        return jnp.where(sub < 3, e[:, :128], rest)[:4]

    def sources(buf, base, at, radius, center):
        rest = buf[pl.ds(base, 8), 3, :]
        turned = [rest] + [pltpu.roll(rest, 32 * m, 1) for m in range(1, 4)]
        place = (lane // 32) == (sub % 4)
        for k in range(3):
            f = buf[pl.ds(base, 8), k, :]
            r = turned[(0 - k) % 4]
            for j in range(1, 4):
                r = jnp.where(sub % 4 == j, turned[(j - k) % 4], r)
            r = jnp.where(place, r, 0.0) * VISCOSITY
            at_f = at + (3 + k) * 16
            src_ref[at_f : at_f + 8, :] = f * VISCOSITY
            src_ref[at_f + 8 : at_f + 9, :] = jnp.sum(r[:4], axis=0, keepdims=True)
            src_ref[at_f + 9 : at_f + 10, :] = jnp.sum(r[4:], axis=0, keepdims=True)
            c = jnp.broadcast_to(rest[:, 96 + k : 97 + k] - center[k], (8, 128))
            pc = jnp.where(place, c, 0.0)
            at_c = at + k * 16
            src_ref[at_c : at_c + 8, :] = c + radius * box_rows[k : k + 1, :128]
            more = radius * box_rows[k : k + 1, 128:]
            src_ref[at_c + 8 : at_c + 9, :] = jnp.sum(pc[:4], axis=0, keepdims=True) + more
            src_ref[at_c + 9 : at_c + 10, :] = jnp.sum(pc[4:], axis=0, keepdims=True) + more

    def far(at):
        def one(i, c):
            rows = [pl.ds(pl.multiple_of(k * QP + i * 16, 16), 16) for k in range(3)]
            t = [targets[r, :] for r in rows]
            acc = tuple(acc_ref[r, :] for r in rows)
            tiles = [src_ref[at + 16 * k : at + 16 * k + 16, :] for k in range(6)]
            for j in range(10):
                acc = pair(t, [row_of(x, j, 16) for x in tiles], acc)
            for r, a in zip(rows, acc):
                acc_ref[r, :] = a
            return c

        lax.fori_loop(0, QP // 16, one, 0)

    pts = [
        jnp.concatenate([pos_ref[k], jnp.zeros((4, PT), F32)], axis=0) for k in range(3)
    ]
    for step in range(STEPS):
        ca0, cb0 = step * 64, step * 64
        cells = ca_buf.at[pl.ds(pl.multiple_of(ca0 + mx * 16, 8), 16), :]

        def send_cells():
            for i in (2, 1, 3):
                push(cells, cells, CA + step, {"dev": lax.rem(mx + i, NX) * NY + my})

        ca_buf[pl.ds(pl.multiple_of(ca0 + mx * 16, 8), 16), :] = own_cells(pts)
        if step > 0:
            send_cells()
        acc_ref[...] = jnp.zeros_like(acc_ref)
        cents, forces = membrane(pts)
        center = [jnp.sum(c[:4], axis=0, keepdims=True) * 0.25 for c in cents]
        total = [jnp.sum(f[:4], axis=0, keepdims=True) for f in forces]
        m3 = row8 % 3
        fs = jnp.where(m3 == 0, total[0], jnp.where(m3 == 1, total[1], total[2]))
        fh, fl = halves(fs)
        msg = message(dot_t(fh, up_hi[...]) + dot_t(fl, up_hi[...]) + dot_t(fh, up_lo[...]), center)
        eq_msg[step] = msg

        if step == 0:
            pl.semaphore_wait(barrier, ND - 1 + NG - 1)
        send_boxes(step)
        mine = pl.ds(pl.multiple_of(my * 8, 8), 8)
        if step == 0:
            send_cells()
            for i in (4, 3, 5, 2, 6, 1, 7):
                y = lax.rem(my + i, NY)
                push(
                    rq_send.at[pl.ds(pl.multiple_of(y * 8, 8), 8), :],
                    rq_recv.at[mine, :],
                    RQ,
                    {"dev": mx * NY + y},
                )
            rq_recv[mine, :] = rq_send[mine, :]

        def box_class(c):
            sources(eq_buf, step * 32 + 8 * c, c * 96, DEVICE_RADIUS, center)

        def wait_boxes(c):
            n = 7 if c == 3 else 8
            arrived(eq_buf.at[pl.ds(step * 32 + 8 * c, n)], EQ + 4 * step + c)

        def wait_groups(c):
            n = 7 if c == 2 else 8
            arrived(gp_buf.at[pl.ds(step * 24 + 8 * c, n)], GP + 3 * step + c)

        def group_class(c):
            wait_groups(c)
            sources(gp_buf, step * 24 + 8 * c, (4 + c) * 96, GROUP_RADIUS, center)
            far((4 + c) * 96)

        wait_boxes(0)
        box_class(0)
        far(0)
        if step == 0:
            arrived(rq_recv.at[pl.ds(0, 56), :], RQ)
        arrived(ca_buf.at[pl.ds(ca0, 48), :], CA + step)

        pick = rq_recv[:, :64] == lax.broadcasted_iota(jnp.int32, (64, 64), 1)
        pick = jnp.where(pick, 1.0, 0.0).astype(BF)
        cells = ca_buf[ca0 : ca0 + 64, :]
        c1 = cells.astype(BF)
        cells = cells - c1.astype(F32)
        c2 = cells.astype(BF)
        c3 = (cells - c2.astype(F32)).astype(BF)
        cb_send[cb0 : cb0 + 64, :] = (dot(pick, c1) + dot(pick, c2)) + dot(pick, c3)
        own_b = pl.ds(pl.multiple_of(cb0 + my * 8, 8), 8)
        for i in (4, 3, 5, 2, 6, 1, 7):
            y = lax.rem(my + i, NY)
            push(
                cb_send.at[pl.ds(pl.multiple_of(cb0 + y * 8, 8), 8), :],
                cb_recv.at[own_b, :],
                CB + step,
                {"dev": mx * NY + y},
            )
        cb_recv[own_b, :] = cb_send[own_b, :]

        for c in (1, 2):
            wait_boxes(c)
            box_class(c)
            far(c * 96)
        wait_boxes(3)
        parts = [eq_buf[step * 32 + i] for i in range(ND - 1)] + [msg]
        while len(parts) > 1:
            parts = [a + b for a, b in zip(parts[::2], parts[1::2])]
        tile = parts[0]
        last = tile[3:4, :]
        main = jnp.concatenate([tile, jnp.zeros((4, 128), F32)], axis=0)
        tail = jnp.broadcast_to(last, (8, 128))
        rest = tail
        for k in range(1, 3):
            rest = jnp.where(sub == k, pltpu.roll(tail, 128 - 32 * k, 1), rest)
        rest = rest[:, :32]
        middle = [last[:, 96 + k : 97 + k] * (1.0 / ND) for k in range(3)]
        group = mm(main, mm_hi[:128], mm_lo[:128]) + mm(rest, mm_hi[128:], mm_lo[128:])
        gp_msg[step] = message(group, middle)
        send_groups(step)

        box_class(3)
        far(3 * 96)

        arrived(cb_recv.at[pl.ds(cb0, 56), :], CB + step)
        near = cb_recv[cb0 : cb0 + 8, :]
        for y in range(1, NY):
            near = near + cb_recv[cb0 + 8 * y : cb0 + 8 * y + 8, :]
        npts = [jnp.where(row8 == 0, near[k : k + 1], near[4 + k : 5 + k]) for k in range(3)]
        _, nforces = membrane(npts)
        for s in range(2):
            for k in range(3):
                near_src[s * 8 + k : s * 8 + k + 1, :PT] = near[4 * s + k : 4 * s + k + 1]
                near_src[s * 8 + 3 + k : s * 8 + 4 + k, :PT] = nforces[k][s : s + 1] * VISCOSITY
                near_rows[4 * s + k : 4 * s + k + 1, :PT] = jnp.sum(
                    jnp.where(row8 == t_of[s], pts[k], 0.0), axis=0, keepdims=True
                )
        near_cols[...] = near_rows[...].T

        def near_block(i, c):
            at = pl.multiple_of(i * 32, 32)
            cols = near_cols[pl.ds(at, 32), :]
            for s in range(2):
                t = [
                    jnp.broadcast_to(cols[:, 4 * s + k : 4 * s + k + 1], (32, 128))
                    for k in range(3)
                ]
                acc = tuple(jnp.zeros((32, 128), F32) for k in range(3))
                for q in range(PP // 128):
                    src = near_src[s * 8 : s * 8 + 8, q * 128 : q * 128 + 128]
                    acc = pair(t, [row_of(src, j, 32) for j in range(6)], acc)
                for k in range(3):
                    near_acc[pl.ds((3 * s + k) * PP + at, 32), :] = acc[k]
            return c

        lax.fori_loop(0, PT // 32, near_block, 0)
        nv = []
        for i in range(6):
            summed = jnp.sum(near_acc[i * PP : (i + 1) * PP, :].T, axis=0, keepdims=True)
            nv.append(summed[:, :PT])

        for c in range(3):
            group_class(c)
        ones = jnp.ones((16, 128), BF)
        checks = []
        for k in range(3):
            ah, al = halves(acc_ref[k * QP : k * QP + Q, :])
            dims = (((1,), (1,)), ((), ()))
            checks.append(
                (
                    lax.dot_general(ones, ah, dims, preferred_element_type=F32)
                    + lax.dot_general(ones, al, dims, preferred_element_type=F32)
                )[:8]
            )
        surface = mm(jnp.concatenate(checks, axis=0), dn_hi, dn_lo)

        for k in range(3):
            v = surface[8 * k : 8 * k + 8]
            for s in range(2):
                v = v + jnp.where((row8 == t_of[s]) & used[s], nv[3 * s + k], 0.0)
            pts[k] = pts[k] + TIME_STEP * v
            if step == STEPS - 1:
                vel_ref[k] = v[:4]
                new_ref[k] = pts[k][:4]

    for step in range(STEPS):
        left(eq_buf.at[pl.ds(0, 31)], EQ + 4 * step)
        left(gp_buf.at[pl.ds(0, 23)], GP + 3 * step)
        left(ca_buf.at[pl.ds(0, 48), :], CA + step)
        left(cb_send.at[pl.ds(0, 56), :], CB + step)
    left(rq_send.at[pl.ds(0, 56), :], RQ)


def body(
    positions,
    rest_shape,
    stiffness,
    up_map,
    down_map,
    m2m,
    box_template,
    near_target,
    near_owner,
    near_cell,
    near_count,
):
    vmem = pl.BlockSpec(memory_space=pltpu.VMEM)
    hbm = pl.BlockSpec(memory_space=pltpu.HBM)
    arrays = (
        near_target,
        near_owner,
        near_cell,
        near_count,
        positions,
        rest_shape,
        stiffness,
        up_map.T,
        m2m,
        down_map,
        box_template,
    )
    shape = jax.ShapeDtypeStruct(positions.shape, F32)
    return pl.pallas_call(
        kernel,
        out_shape=(shape, shape),
        in_specs=[hbm] * 11,
        out_specs=(vmem, vmem),
        scratch_shapes=[pltpu.SMEM(a.shape, a.dtype) for a in arrays[:4]]
        + [pltpu.VMEM(a.shape, a.dtype) for a in arrays[4:]]
        + [
            pltpu.VMEM((PT, PT), BF),
            pltpu.VMEM((PT, PT), BF),
            pltpu.VMEM((256, PT), BF),
            pltpu.VMEM((256, PT), BF),
            pltpu.VMEM((QP, 256), BF),
            pltpu.VMEM((QP, 256), BF),
            pltpu.VMEM((Q, PT), BF),
            pltpu.VMEM((Q, PT), BF),
            pltpu.VMEM((8, 256), F32),
            pltpu.VMEM((3 * QP, 128), F32),
            pltpu.VMEM((3 * QP, 128), F32),
            pltpu.VMEM((STEPS, 4, 128), F32),
            pltpu.VMEM((STEPS, 4, 128), F32),
            pltpu.VMEM((STEPS * 32, 4, 128), F32),
            pltpu.VMEM((STEPS * 24, 4, 128), F32),
            pltpu.VMEM((STEPS * 64, PT), F32),
            pltpu.VMEM((STEPS * 64, PT), F32),
            pltpu.VMEM((STEPS * 64, PT), F32),
            pltpu.VMEM((64, 128), jnp.int32),
            pltpu.VMEM((64, 128), jnp.int32),
            pltpu.VMEM((7 * 96, 128), F32),
            pltpu.VMEM((16, PP), F32),
            pltpu.VMEM((8, PP), F32),
            pltpu.VMEM((PP, 8), F32),
            pltpu.VMEM((6 * PP, 128), F32),
            pltpu.SemaphoreType.DMA((19,)),
            pltpu.SemaphoreType.DMA((19,)),
            pltpu.SemaphoreType.DMA((11,)),
        ],
        compiler_params=pltpu.CompilerParams(
            collective_id=0, has_side_effects=True
        ),
    )(*arrays)


def solution(mesh):
    return jax.shard_map(
        body,
        mesh=mesh,
        in_specs=(
            P(None, ("grp", "dev"), None),
            P(),
            P(),
            P(),
            P(),
            P(),
            P(),
            P(("grp", "dev"), None),
            P(("grp", "dev"), None),
            P(("grp", "dev"), None),
            P(("grp", "dev")),
        ),
        out_specs=(P(None, ("grp", "dev"), None), P(None, ("grp", "dev"), None)),
        check_vma=False,
    )
```

```python
import functools

import jax
import jax.numpy as jnp
from jax import lax
from jax.experimental import pallas as pl
from jax.experimental.pallas import tpu as pltpu
from jax.sharding import PartitionSpec as P

STEPS = 2
EPS = 0.25
VISCOSITY = 0.039788735772973836
TIME_STEP = 0.1
SKALAK_HARDEN = 2.0
CHECK_RADIUS = 1.0
DEVICE_RADIUS = 1.5
GROUP_RADIUS = 6.0

NG = 24
ND = 32
NX = 4
NY = 8
PT = 544
PP = 640
Q = 152
F32 = jnp.float32
BF = jnp.bfloat16
MESH = pl.DeviceIdType.MESH

QP = 160
DEV_OFF = sorted(
    [(x, y) for x in range(NX) for y in range(NY) if (x, y) != (0, 0)],
    key=lambda o: (min(o[0], NX - o[0]) + min(o[1], NY - o[1]), o),
)
GRP_OFF = sorted(range(1, NG), key=lambda o: (min(o, NG - o), o))
DEV_SLOT = {o: i for i, o in enumerate(DEV_OFF)}
GRP_SLOT = {o: i for i, o in enumerate(GRP_OFF)}
EQ, GP, CA, CB, RQ = 0, 8, 14, 16, 18


def halves(w):
    hi = w.astype(BF)
    return hi, (w - hi.astype(F32)).astype(BF)


def dot(a, b):
    return jnp.dot(a, b, preferred_element_type=F32)


def dot_t(a, b):
    return lax.dot_general(a, b, (((1,), (1,)), ((), ())), preferred_element_type=F32)


def mm(a, hi, lo):
    ah, al = halves(a)
    return dot(ah, hi[...]) + dot(al, hi[...]) + dot(ah, lo[...])


def pair(t, s, acc):
    tx, ty, tz = t
    sx, sy, sz, fx, fy, fz = s
    dx, dy, dz = tx - sx, ty - sy, tz - sz
    rs = lax.rsqrt(dx * dx + dy * dy + (dz * dz + EPS))
    b = rs * rs * rs
    direct = rs + EPS * b
    proj = (dx * fx + dy * fy + dz * fz) * b
    return (
        acc[0] + (direct * fx + proj * dx),
        acc[1] + (direct * fy + proj * dy),
        acc[2] + (direct * fz + proj * dz),
    )


def row_of(tile, j, rows):
    return jnp.broadcast_to(tile[j : j + 1, :], (rows, 128))


def kernel(
    *refs
):
    inputs, (new_ref, vel_ref), local = refs[:11], refs[11:13], refs[13:24]
    (
        st_hi,
        st_lo,
        up_hi,
        up_lo,
        mm_hi,
        mm_lo,
        dn_hi,
        dn_lo,
        box_rows,
        targets,
        acc_ref,
        eq_msg,
        gp_msg,
        eq_buf,
        gp_buf,
        ca_buf,
        cb_send,
        cb_recv,
        rq_send,
        rq_recv,
        src_ref,
        near_src,
        near_rows,
        near_cols,
        near_acc,
        send_sem,
        recv_sem,
        load_sem,
    ) = refs[24:]
    loads = [
        pltpu.make_async_copy(a, b, load_sem.at[i])
        for i, (a, b) in enumerate(zip(inputs, local))
    ]
    for load in loads:
        load.start()
    (
        near_target,
        near_owner,
        near_cell,
        near_count,
        pos_ref,
        rest_ref,
        stiff_ref,
        up_ref,
        m2m_ref,
        down_ref,
        box_ref,
    ) = local
    me = lax.axis_index("dev")
    grp = lax.axis_index("grp")
    mx = me // NY
    my = me % NY

    barrier = pltpu.get_barrier_semaphore()

    def greet(axis, own, count):
        def one(i, c):
            pl.semaphore_signal(
                barrier, inc=1, device_id={axis: lax.rem(own + i, count)}, device_id_type=MESH
            )
            return c

        lax.fori_loop(1, count, one, 0)

    greet("dev", me, ND)
    greet("grp", grp, NG)

    def push(src, dst, sem, device, arrival=None):
        pltpu.make_async_remote_copy(
            src_ref=src,
            dst_ref=dst,
            send_sem=send_sem.at[sem],
            recv_sem=recv_sem.at[sem if arrival is None else arrival],
            device_id=device,
            device_id_type=MESH,
        ).start()

    def arrived(ref, sem):
        pltpu.make_async_copy(ref, ref, recv_sem.at[sem]).wait()

    def left(ref, sem):
        pltpu.make_async_copy(ref, ref, send_sem.at[sem]).wait()

    def send_boxes(step):
        for x, y in reversed(DEV_OFF):
            slot = DEV_SLOT[((NX - x) % NX, (NY - y) % NY)]
            peer = lax.rem(mx + x, NX) * NY + lax.rem(my + y, NY)
            push(
                eq_msg.at[step],
                eq_buf.at[step * 32 + slot],
                EQ + 4 * step,
                {"dev": peer},
                EQ + 4 * step + slot // 8,
            )

    def send_groups(step):
        for o in reversed(GRP_OFF):
            slot = GRP_SLOT[NG - o]
            push(
                gp_msg.at[step],
                gp_buf.at[step * 24 + slot],
                GP + 3 * step,
                {"grp": lax.rem(grp + o, NG)},
                GP + 3 * step + slot // 8,
            )

    for load in loads:
        load.wait()

    def spread(a, axis):
        shape = list(a.shape)
        shape[axis] = 8
        gap = jnp.zeros(shape, F32)
        main, rest = (a[:, :128], a[:, 128:]) if axis else (a[:128], a[128:])
        return jnp.concatenate([main] + [rest, gap] * 4, axis=axis)

    st_hi[...], st_lo[...] = halves(stiff_ref[...])
    up_hi[...], up_lo[...] = halves(spread(up_ref[...], 0))
    mm_hi[0:Q, :], mm_lo[0:Q, :] = halves(spread(m2m_ref[...], 1))
    mm_hi[Q:, :] = jnp.zeros((8, 256), BF)
    mm_lo[Q:, :] = jnp.zeros((8, 256), BF)
    dn_hi[...], dn_lo[...] = halves(down_ref[...])
    box_rows[...] = jnp.zeros_like(box_rows)
    box_rows[0:3, 0:Q] = box_ref[...]
    cols = box_rows[...].T
    for k in range(3):
        targets[k * QP : (k + 1) * QP, :] = jnp.broadcast_to(
            CHECK_RADIUS * cols[:QP, k : k + 1], (QP, 128)
        )
    box_rows[0:3, :] = spread(box_ref[...], 1)
    for step in range(STEPS):
        eq_buf[step * 32 + 31] = jnp.zeros((4, 128), F32)
        gp_buf[step * 24 + 23] = jnp.zeros((4, 128), F32)
    near_src[...] = jnp.zeros_like(near_src)
    near_rows[...] = jnp.zeros_like(near_rows)
    near_acc[...] = jnp.zeros_like(near_acc)

    sub = lax.broadcasted_iota(jnp.int32, (8, 128), 0)
    lane = lax.broadcasted_iota(jnp.int32, (8, 128), 1)
    row8 = lax.broadcasted_iota(jnp.int32, (8, PT), 0)
    count = near_count[0]
    t_of = [near_target[0, s] for s in range(2)]
    used = [s < count for s in range(2)]

    want, from_y = [], []
    for s in range(2):
        owner = near_owner[0, s]
        want.append((owner // NY) * 16 + near_cell[0, s])
        from_y.append(jnp.where(used[s], owner % NY, -1))
    kk = sub % 4
    slot_want = jnp.where(sub < 4, want[0], want[1]) + 4 * kk
    slot_y = jnp.where(sub < 4, from_y[0], from_y[1])
    for y in range(NY):
        rq_send[y * 8 : (y + 1) * 8, :] = jnp.where((slot_y == y) & (kk < 3), slot_want, -1)

    def membrane(pts):
        cents, strain = [], []
        for k in range(3):
            c = jnp.sum(pts[k], axis=1, keepdims=True) * (1.0 / PT)
            cents.append(c)
            strain.append(pts[k] - c - rest_ref[k : k + 1, :])
        flat = jnp.concatenate(strain, axis=0)
        hi = flat.astype(BF).astype(F32)
        both = jnp.concatenate([hi, flat - hi], axis=0).astype(BF)
        first = dot(both, st_hi[...])
        linear = first[:24] + first[24:] + dot(both[:32], st_lo[...])[:24]
        lin = [linear[8 * k : 8 * k + 8] for k in range(3)]
        stretch = lin[0] * lin[0] + lin[1] * lin[1] + lin[2] * lin[2]
        harden = 1.0 + SKALAK_HARDEN * stretch / (1.0 + stretch)
        return cents, [-l * harden for l in lin]

    def own_cells(pts):
        return jnp.concatenate([p[:4] for p in pts] + [jnp.zeros((4, PT), F32)], axis=0)

    def message(e, center):
        rest = jnp.where(lane == 96, center[0], jnp.where(lane == 97, center[1], center[2]))
        for k in range(3):
            rest = jnp.where(lane // 32 == k, e[k : k + 1, 128:], rest)
        return jnp.where(sub < 3, e[:, :128], rest)[:4]

    def sources(buf, base, at, radius, center):
        rest = buf[pl.ds(base, 8), 3, :]
        turned = [rest] + [pltpu.roll(rest, 32 * m, 1) for m in range(1, 4)]
        place = (lane // 32) == (sub % 4)
        for k in range(3):
            f = buf[pl.ds(base, 8), k, :]
            r = turned[(0 - k) % 4]
            for j in range(1, 4):
                r = jnp.where(sub % 4 == j, turned[(j - k) % 4], r)
            r = jnp.where(place, r, 0.0) * VISCOSITY
            at_f = at + (3 + k) * 16
            src_ref[at_f : at_f + 8, :] = f * VISCOSITY
            src_ref[at_f + 8 : at_f + 9, :] = jnp.sum(r[:4], axis=0, keepdims=True)
            src_ref[at_f + 9 : at_f + 10, :] = jnp.sum(r[4:], axis=0, keepdims=True)
            c = jnp.broadcast_to(rest[:, 96 + k : 97 + k] - center[k], (8, 128))
            pc = jnp.where(place, c, 0.0)
            at_c = at + k * 16
            src_ref[at_c : at_c + 8, :] = c + radius * box_rows[k : k + 1, :128]
            more = radius * box_rows[k : k + 1, 128:]
            src_ref[at_c + 8 : at_c + 9, :] = jnp.sum(pc[:4], axis=0, keepdims=True) + more
            src_ref[at_c + 9 : at_c + 10, :] = jnp.sum(pc[4:], axis=0, keepdims=True) + more

    def far(at):
        def one(i, c):
            rows = [pl.ds(pl.multiple_of(k * QP + i * 16, 16), 16) for k in range(3)]
            t = [targets[r, :] for r in rows]
            acc = tuple(acc_ref[r, :] for r in rows)
            tiles = [src_ref[at + 16 * k : at + 16 * k + 16, :] for k in range(6)]
            for j in range(10):
                acc = pair(t, [row_of(x, j, 16) for x in tiles], acc)
            for r, a in zip(rows, acc):
                acc_ref[r, :] = a
            return c

        lax.fori_loop(0, QP // 16, one, 0)

    pts = [
        jnp.concatenate([pos_ref[k], jnp.zeros((4, PT), F32)], axis=0) for k in range(3)
    ]
    for step in range(STEPS):
        ca0, cb0 = step * 64, step * 64
        cells = ca_buf.at[pl.ds(pl.multiple_of(ca0 + mx * 16, 8), 16), :]

        def send_cells():
            for i in (2, 1, 3):
                push(cells, cells, CA + step, {"dev": lax.rem(mx + i, NX) * NY + my})

        ca_buf[pl.ds(pl.multiple_of(ca0 + mx * 16, 8), 16), :] = own_cells(pts)
        if step > 0:
            send_cells()
        acc_ref[...] = jnp.zeros_like(acc_ref)
        cents, forces = membrane(pts)
        center = [jnp.sum(c[:4], axis=0, keepdims=True) * 0.25 for c in cents]
        total = [jnp.sum(f[:4], axis=0, keepdims=True) for f in forces]
        m3 = row8 % 3
        fs = jnp.where(m3 == 0, total[0], jnp.where(m3 == 1, total[1], total[2]))
        fh, fl = halves(fs)
        msg = message(dot_t(fh, up_hi[...]) + dot_t(fl, up_hi[...]) + dot_t(fh, up_lo[...]), center)
        eq_msg[step] = msg

        if step == 0:
            pl.semaphore_wait(barrier, ND - 1 + NG - 1)
        send_boxes(step)
        mine = pl.ds(pl.multiple_of(my * 8, 8), 8)
        if step == 0:
            send_cells()
            for i in (4, 3, 5, 2, 6, 1, 7):
                y = lax.rem(my + i, NY)
                push(
                    rq_send.at[pl.ds(pl.multiple_of(y * 8, 8), 8), :],
                    rq_recv.at[mine, :],
                    RQ,
                    {"dev": mx * NY + y},
                )
            rq_recv[mine, :] = rq_send[mine, :]

        def box_class(c):
            sources(eq_buf, step * 32 + 8 * c, c * 96, DEVICE_RADIUS, center)

        def wait_boxes(c):
            n = 7 if c == 3 else 8
            arrived(eq_buf.at[pl.ds(step * 32 + 8 * c, n)], EQ + 4 * step + c)

        def wait_groups(c):
            n = 7 if c == 2 else 8
            arrived(gp_buf.at[pl.ds(step * 24 + 8 * c, n)], GP + 3 * step + c)

        def group_class(c):
            wait_groups(c)
            sources(gp_buf, step * 24 + 8 * c, (4 + c) * 96, GROUP_RADIUS, center)
            far((4 + c) * 96)

        if step == 0:
            arrived(rq_recv.at[pl.ds(0, 56), :], RQ)
        arrived(ca_buf.at[pl.ds(ca0, 48), :], CA + step)

        pick = rq_recv[:, :64] == lax.broadcasted_iota(jnp.int32, (64, 64), 1)
        pick = jnp.where(pick, 1.0, 0.0).astype(BF)
        cells = ca_buf[ca0 : ca0 + 64, :]
        c1 = cells.astype(BF)
        cells = cells - c1.astype(F32)
        c2 = cells.astype(BF)
        c3 = (cells - c2.astype(F32)).astype(BF)
        cb_send[cb0 : cb0 + 64, :] = (dot(pick, c1) + dot(pick, c2)) + dot(pick, c3)
        own_b = pl.ds(pl.multiple_of(cb0 + my * 8, 8), 8)
        for i in (4, 3, 5, 2, 6, 1, 7):
            y = lax.rem(my + i, NY)
            push(
                cb_send.at[pl.ds(pl.multiple_of(cb0 + y * 8, 8), 8), :],
                cb_recv.at[own_b, :],
                CB + step,
                {"dev": mx * NY + y},
            )
        cb_recv[own_b, :] = cb_send[own_b, :]

        for c in range(4):
            wait_boxes(c)
        parts = [eq_buf[step * 32 + i] for i in range(ND - 1)] + [msg]
        while len(parts) > 1:
            parts = [a + b for a, b in zip(parts[::2], parts[1::2])]
        tile = parts[0]
        last = tile[3:4, :]
        main = jnp.concatenate([tile, jnp.zeros((4, 128), F32)], axis=0)
        tail = jnp.broadcast_to(last, (8, 128))
        rest = tail
        for k in range(1, 3):
            rest = jnp.where(sub == k, pltpu.roll(tail, 128 - 32 * k, 1), rest)
        rest = rest[:, :32]
        middle = [last[:, 96 + k : 97 + k] * (1.0 / ND) for k in range(3)]
        group = mm(main, mm_hi[:128], mm_lo[:128]) + mm(rest, mm_hi[128:], mm_lo[128:])
        gp_msg[step] = message(group, middle)
        send_groups(step)

        for c in range(4):
            box_class(c)
            far(c * 96)
        for c in range(2):
            group_class(c)

        arrived(cb_recv.at[pl.ds(cb0, 56), :], CB + step)
        near = cb_recv[cb0 : cb0 + 8, :]
        for y in range(1, NY):
            near = near + cb_recv[cb0 + 8 * y : cb0 + 8 * y + 8, :]
        npts = [jnp.where(row8 == 0, near[k : k + 1], near[4 + k : 5 + k]) for k in range(3)]
        _, nforces = membrane(npts)
        for s in range(2):
            for k in range(3):
                near_src[s * 8 + k : s * 8 + k + 1, :PT] = near[4 * s + k : 4 * s + k + 1]
                near_src[s * 8 + 3 + k : s * 8 + 4 + k, :PT] = nforces[k][s : s + 1] * VISCOSITY
                near_rows[4 * s + k : 4 * s + k + 1, :PT] = jnp.sum(
                    jnp.where(row8 == t_of[s], pts[k], 0.0), axis=0, keepdims=True
                )
        near_cols[...] = near_rows[...].T

        def near_block(i, c):
            at = pl.multiple_of(i * 32, 32)
            cols = near_cols[pl.ds(at, 32), :]
            for s in range(2):
                t = [
                    jnp.broadcast_to(cols[:, 4 * s + k : 4 * s + k + 1], (32, 128))
                    for k in range(3)
                ]
                acc = tuple(jnp.zeros((32, 128), F32) for k in range(3))
                for q in range(PP // 128):
                    src = near_src[s * 8 : s * 8 + 8, q * 128 : q * 128 + 128]
                    acc = pair(t, [row_of(src, j, 32) for j in range(6)], acc)
                for k in range(3):
                    near_acc[pl.ds((3 * s + k) * PP + at, 32), :] = acc[k]
            return c

        lax.fori_loop(0, PT // 32, near_block, 0)
        nv = []
        for i in range(6):
            summed = jnp.sum(near_acc[i * PP : (i + 1) * PP, :].T, axis=0, keepdims=True)
            nv.append(summed[:, :PT])

        group_class(2)
        ones = jnp.ones((16, 128), BF)
        checks = []
        for k in range(3):
            ah, al = halves(acc_ref[k * QP : k * QP + Q, :])
            dims = (((1,), (1,)), ((), ()))
            checks.append(
                (
                    lax.dot_general(ones, ah, dims, preferred_element_type=F32)
                    + lax.dot_general(ones, al, dims, preferred_element_type=F32)
                )[:8]
            )
        surface = mm(jnp.concatenate(checks, axis=0), dn_hi, dn_lo)

        for k in range(3):
            v = surface[8 * k : 8 * k + 8]
            for s in range(2):
                v = v + jnp.where((row8 == t_of[s]) & used[s], nv[3 * s + k], 0.0)
            pts[k] = pts[k] + TIME_STEP * v
            if step == STEPS - 1:
                vel_ref[k] = v[:4]
                new_ref[k] = pts[k][:4]

    for step in range(STEPS):
        left(eq_buf.at[pl.ds(0, 31)], EQ + 4 * step)
        left(gp_buf.at[pl.ds(0, 23)], GP + 3 * step)
        left(ca_buf.at[pl.ds(0, 48), :], CA + step)
        left(cb_send.at[pl.ds(0, 56), :], CB + step)
    left(rq_send.at[pl.ds(0, 56), :], RQ)


def settle(new_ref, vel_ref, new_out, vel_out):
    new_out[...] = new_ref[...]
    vel_out[...] = vel_ref[...]


def body(
    positions,
    rest_shape,
    stiffness,
    up_map,
    down_map,
    m2m,
    box_template,
    near_target,
    near_owner,
    near_cell,
    near_count,
):
    vmem = pl.BlockSpec(memory_space=pltpu.VMEM)
    hbm = pl.BlockSpec(memory_space=pltpu.HBM)
    arrays = (
        near_target,
        near_owner,
        near_cell,
        near_count,
        positions,
        rest_shape,
        stiffness,
        up_map.T,
        m2m,
        down_map,
        box_template,
    )
    shape = jax.ShapeDtypeStruct(positions.shape, F32)
    ends = pl.pallas_call(
        kernel,
        out_shape=(shape, shape),
        in_specs=[hbm] * 11,
        out_specs=(vmem, vmem),
        scratch_shapes=[pltpu.SMEM(a.shape, a.dtype) for a in arrays[:4]]
        + [pltpu.VMEM(a.shape, a.dtype) for a in arrays[4:]]
        + [
            pltpu.VMEM((PT, PT), BF),
            pltpu.VMEM((PT, PT), BF),
            pltpu.VMEM((256, PT), BF),
            pltpu.VMEM((256, PT), BF),
            pltpu.VMEM((QP, 256), BF),
            pltpu.VMEM((QP, 256), BF),
            pltpu.VMEM((Q, PT), BF),
            pltpu.VMEM((Q, PT), BF),
            pltpu.VMEM((8, 256), F32),
            pltpu.VMEM((3 * QP, 128), F32),
            pltpu.VMEM((3 * QP, 128), F32),
            pltpu.VMEM((STEPS, 4, 128), F32),
            pltpu.VMEM((STEPS, 4, 128), F32),
            pltpu.VMEM((STEPS * 32, 4, 128), F32),
            pltpu.VMEM((STEPS * 24, 4, 128), F32),
            pltpu.VMEM((STEPS * 64, PT), F32),
            pltpu.VMEM((STEPS * 64, PT), F32),
            pltpu.VMEM((STEPS * 64, PT), F32),
            pltpu.VMEM((64, 128), jnp.int32),
            pltpu.VMEM((64, 128), jnp.int32),
            pltpu.VMEM((7 * 96, 128), F32),
            pltpu.VMEM((16, PP), F32),
            pltpu.VMEM((8, PP), F32),
            pltpu.VMEM((PP, 8), F32),
            pltpu.VMEM((6 * PP, 128), F32),
            pltpu.SemaphoreType.DMA((19,)),
            pltpu.SemaphoreType.DMA((19,)),
            pltpu.SemaphoreType.DMA((11,)),
        ],
        compiler_params=pltpu.CompilerParams(
            collective_id=0, has_side_effects=True
        ),
    )(*arrays)
    return pl.pallas_call(settle, out_shape=(shape, shape))(*ends)


def solution(mesh):
    return jax.shard_map(
        body,
        mesh=mesh,
        in_specs=(
            P(None, ("grp", "dev"), None),
            P(),
            P(),
            P(),
            P(),
            P(),
            P(),
            P(("grp", "dev"), None),
            P(("grp", "dev"), None),
            P(("grp", "dev"), None),
            P(("grp", "dev")),
        ),
        out_specs=(P(None, ("grp", "dev"), None), P(None, ("grp", "dev"), None)),
        check_vma=False,
    )
```
